512 devices in a mesh: grp: 2 (over y), seq: 128 (over z, x), head: 2 (over core).
Axes of the slice: x: 8, y: 2, z: 16, core: 2. Of those that a mesh axis runs over, the one named last changes fastest.
The devices are a block of a 8x8x16 slice.
Arguments:
- key_cache: bfloat16 [4, 1024, 128, 1024], P('grp', ('seq', 'head')), parts along dimension 0, may hold values from -160 to 160, as said below
- value_cache: bfloat16 [4, 1024, 128, 1024], P('grp', ('seq', 'head')), parts along dimension 0, may hold values from -16 to 16, as said below
- query: bfloat16 [4, 4096], P('grp', 'head'), parts along dimension 0, may hold values from -48 to 48, as said below
- lengths: int32 [4], P('grp'), parts along dimension 0, may hold values from 128 to 131072, as said below
- block_map: int32 [4, 1024], P('grp'), parts along dimension 0, may hold values from 0 to 1023, each once within a row
Outputs:
- attended: bfloat16 [4, 4096], P('grp', 'head'), parts along dimension 0
The draws below stay inside these ranges and needn't reach their ends.
There are 2 independent parts, one for each index of `grp`. The reference program is written for one: setup_inputs(seed, part) draws one part's arguments, and reference() takes and returns one part's arrays. A program takes and returns all parts, laid end to end along the dimension named above; each array names one. Nothing has to cross between parts.
Inputs may be any that keep to these rules, and one draw needn't show every extreme that they name: `lengths`: every length is a multiple of 128; in every draw some request has length 131072. `key_cache`: finite entries, drawn afresh for every request, block, token and channel. `value_cache`: finite entries, drawn afresh for every request, block, token and channel. `query`: finite entries, drawn afresh for every request, head and channel.
All inputs are finite; a program needn't handle non-finite values.
Results may differ from the reference program's by a relative error of at most 0.0055.
Values may be sent and summed in bfloat16 or wider, within the bound.
No kernel may reach another device: no remote copies, remote signals or barrier semaphores. Data moves between devices by JAX's collectives and lax.ppermute only.
A program may use at most 64 MiB of HBM per device.

```python
import jax
import jax.numpy as jnp
from jax import lax

QH = 32
KVH = 8
HD = 128
BLK = 128
BATCH = 2
NBLK = 1024


def layout_terms(key):
    first_key, second_key, third_key = jax.random.split(jax.random.fold_in(key, 11), 3)
    direction = jax.random.normal(first_key, (KVH, HD), jnp.float32)
    direction = direction / jnp.sqrt(jnp.sum(direction * direction, axis=1, keepdims=True))
    coeffs = jax.random.uniform(second_key, (BATCH, NBLK, KVH), jnp.float32, -1.5, 1.5)
    return (direction, coeffs)


def draw_key_cache(key, part):
    direction, coeffs = layout_terms(key)
    shape = (BATCH, NBLK, BLK, KVH, HD)
    noise = jax.random.normal(jax.random.fold_in(key, 21), shape, jnp.float32)
    keys_full = noise + coeffs[:, :, None, :, None] * direction[None, None, None, :, :]
    return keys_full.reshape(BATCH, NBLK, BLK, KVH * HD).astype(jnp.bfloat16)


def draw_value_cache(key, part):
    means = jax.random.normal(jax.random.fold_in(key, 31), (BATCH, NBLK, KVH * HD), jnp.float32)
    noise = 0.5 * jax.random.normal(jax.random.fold_in(key, 32), (BATCH, NBLK, BLK, KVH * HD), jnp.float32)
    return (noise + means[:, :, None, :]).astype(jnp.bfloat16)


def draw_query(key, part):
    direction, coeffs = layout_terms(key)
    noise = jax.random.normal(jax.random.fold_in(key, 41), (BATCH, KVH, QH // KVH, HD), jnp.float32)
    full = noise + 2.0 * HD ** 0.5 * direction[None, :, None, :]
    return full.reshape(BATCH, QH * HD).astype(jnp.bfloat16)


def draw_lengths(key, part):
    first_key, second_key = jax.random.split(jax.random.fold_in(key, 51))
    counts = jax.random.randint(first_key, (BATCH,), 1, NBLK + 1)
    fullest = jax.random.randint(second_key, (), 0, BATCH)
    counts = jnp.where(jnp.arange(BATCH) == fullest, NBLK, counts)
    return (counts * BLK).astype(jnp.int32)


def setup_inputs(seed: int = 0, part: int = 0) -> dict:
    splits = jax.random.split(jax.random.key(seed), 6)
    part_splits = jax.random.split(jax.random.fold_in(splits[5], part), 6)
    key_cache = draw_key_cache(jax.random.fold_in(jax.random.fold_in(splits[5], part), 71), part)
    value_cache = draw_value_cache(jax.random.fold_in(jax.random.fold_in(splits[5], part), 71), part)
    query = draw_query(jax.random.fold_in(jax.random.fold_in(splits[5], part), 71), part)
    lengths = draw_lengths(jax.random.fold_in(jax.random.fold_in(splits[5], part), 71), part)
    block_map = jax.vmap(lambda own: jax.random.permutation(own, NBLK))(jax.random.split(part_splits[4], BATCH)).reshape((BATCH, NBLK)).astype(jnp.int32)
    return dict(key_cache=key_cache, value_cache=value_cache, query=query, lengths=lengths, block_map=block_map)


def reference(key_cache, value_cache, query, lengths, block_map):
    key_rows = key_cache.reshape(BATCH, NBLK * BLK, KVH, HD)
    value_rows = value_cache.reshape(BATCH, NBLK * BLK, KVH, HD)
    live_blocks = block_map < (lengths // BLK)[:, None]
    live_tokens = jnp.repeat(live_blocks, BLK, axis=1)[:, None, :]
    queries = query.reshape(BATCH, KVH, QH // KVH, HD).astype(jnp.float32)
    score_scale = 1.0 / (HD ** 0.5)

    def one_group(group):
        key_portion = key_rows[:, :, group, :].astype(jnp.float32)
        value_portion = value_rows[:, :, group, :].astype(jnp.float32)
        query_portion = queries[:, group]
        logit_scores = jnp.einsum("rcy,rly->rcl", query_portion, key_portion, precision=lax.Precision.HIGHEST) * score_scale
        row_top = jnp.max(jnp.where(live_tokens, logit_scores, jnp.float32(-1e30)), axis=-1)
        expo = jnp.where(live_tokens, jnp.exp(logit_scores - row_top[..., None]), jnp.float32(0.0))
        total = jnp.sum(expo, axis=-1)
        rounded_scores = lax.optimization_barrier(expo.astype(jnp.bfloat16)).astype(jnp.float32)
        summed_values = jnp.einsum("wog,wgn->won", rounded_scores, value_portion, precision=lax.Precision.HIGHEST)
        return summed_values / total[..., None]

    outputs = lax.map(one_group, jnp.arange(KVH, dtype=jnp.int32))
    outputs = jnp.transpose(outputs, (1, 0, 2, 3)).reshape(BATCH, QH * HD)
    return outputs.astype(jnp.bfloat16)
```

```python
import jax
import jax.numpy as jnp
from jax import lax
from jax.experimental import pallas as pl
from jax.experimental.pallas import tpu as pltpu
from jax.sharding import Mesh
from jax.sharding import PartitionSpec as P

QH = 32
KVH = 8
HD = 128
BLK = 128
GROUP = QH // KVH
LOW = -1e30
ROW = ("seq_1", "head")
STATS = 8


def pieces(x):
    first = x.astype(jnp.bfloat16)
    rest = x - first.astype(jnp.float32)
    second = rest.astype(jnp.bfloat16)
    third = (rest - second.astype(jnp.float32)).astype(jnp.bfloat16)
    return first, second, third


def diagonal(rows):
    shape = (rows, HD)
    return lax.broadcasted_iota(jnp.int32, shape, 0) == lax.broadcasted_iota(jnp.int32, shape, 1)


def as_row(column, eye):
    return jnp.sum(jnp.where(eye, column, 0.0), axis=0, keepdims=True)


def as_column(row, eye):
    return jnp.sum(jnp.where(eye, row, 0.0), axis=1, keepdims=True)


def packed(sums, top, total):
    blank = jnp.zeros((STATS - 6, HD), jnp.float32)
    stats = [p.astype(jnp.float32) for p in (*pieces(top), *pieces(total))]
    return jnp.concatenate([sums, *stats, blank], axis=0).astype(jnp.bfloat16)


def attend_kernel(query, lengths, block_map, keys, values, out, key_buf, value_buf, map_buf, len_buf, sems):
    batch, slots = keys.shape[0], keys.shape[1]
    halves = query.shape[0]
    tokens = slots * BLK
    width = keys.shape[3]
    copies = []
    for b in range(batch):
        copies.append(
            (
                pltpu.make_async_copy(keys.at[b], key_buf.at[b], sems.at[0, b]),
                pltpu.make_async_copy(values.at[b], value_buf.at[b], sems.at[1, b]),
            )
        )
    small = (
        pltpu.make_async_copy(block_map, map_buf, sems.at[2, 0]),
        pltpu.make_async_copy(lengths, len_buf, sems.at[2, 1]),
    )
    for copy in small:
        copy.start()
    for pair in copies:
        for copy in pair:
            copy.start()
    for copy in small:
        copy.wait()
    first = lax.axis_index(("seq_0", "seq_1", "head")) * slots
    row_group = lax.broadcasted_iota(jnp.int32, (KVH, width), 0)
    column_group = lax.broadcasted_iota(jnp.int32, (KVH, width), 1) // HD
    own = row_group == column_group
    eye = diagonal(batch * QH // halves)
    sums, tops, totals = [], [], []
    for b in range(batch):
        spread = []
        for i in range(GROUP):
            chunks = []
            for g in range(KVH):
                half, at = divmod(g * GROUP + i, QH // halves)
                chunks.append(query[half, b : b + 1, at * HD : (at + 1) * HD].astype(jnp.float32))
            line = jnp.concatenate(chunks, axis=1)
            spread.append(jnp.where(own, line, 0.0))
        spread = jnp.concatenate(spread, axis=0).astype(jnp.bfloat16)
        limit = len_buf[b] // BLK
        live = jnp.concatenate(
            [
                jnp.full((1, BLK), (map_buf[b, first + j] < limit).astype(jnp.int32))
                for j in range(slots)
            ],
            axis=1,
        )
        live = jnp.broadcast_to(live, (QH, tokens)) > 0
        copies[b][0].wait()
        scores = lax.dot_general(
            spread,
            key_buf[b].reshape(tokens, width),
            (((1,), (1,)), ((), ())),
            preferred_element_type=jnp.float32,
        )
        scores = jnp.where(live, scores * (1.0 / HD**0.5), LOW)
        top = jnp.max(scores, axis=1, keepdims=True)
        expo = jnp.where(live, jnp.exp(scores - top), 0.0)
        total = jnp.sum(expo, axis=1, keepdims=True)
        copies[b][1].wait()
        wide = jnp.dot(
            expo.astype(jnp.bfloat16),
            value_buf[b].reshape(tokens, width),
            preferred_element_type=jnp.float32,
        )
        wide = wide.reshape(GROUP, KVH, width)
        mine = jnp.zeros((GROUP, KVH, HD), jnp.float32)
        for g in range(KVH):
            pick = lax.broadcasted_iota(jnp.int32, mine.shape, 1) == g
            mine = jnp.where(pick, wide[:, :, g * HD : (g + 1) * HD], mine)
        sums.append(mine)
        tops.append(top.reshape(GROUP, KVH, 1))
        totals.append(total.reshape(GROUP, KVH, 1))
    per = KVH // halves
    for half in range(halves):
        part = slice(half * per, (half + 1) * per)

        def gathered(arrays):
            return jnp.concatenate([a[i : i + 1, part].reshape(per, -1) for a in arrays for i in range(GROUP)], axis=0)

        line = packed(
            gathered(sums),
            as_row(gathered(tops), eye),
            as_row(gathered(totals), eye),
        )
        for k in range(out.shape[0]):
            out[k, half] = line


def combined(parts):
    count, rows = parts.shape[0], parts.shape[1] - STATS
    eye = diagonal(rows)
    stats = [parts[:, rows + k, :].astype(jnp.float32) for k in range(6)]
    tops = stats[0] + stats[1] + stats[2]
    totals = stats[3] + stats[4] + stats[5]
    top = jnp.max(tops, axis=0, keepdims=True)
    factors = jnp.exp(tops - top)
    total = jnp.sum(totals * factors, axis=0, keepdims=True)
    sums = jnp.zeros((rows, HD), jnp.float32)
    for n in range(count):
        sums += as_column(factors[n : n + 1], eye) * parts[n, :rows, :].astype(jnp.float32)
    return sums, top, total


def middle_kernel(parts, out):
    line = packed(*combined(parts))
    for k in range(out.shape[0]):
        out[k] = line


def last_kernel(parts, out):
    rows = parts.shape[1] - STATS
    batch = out.shape[0]
    per = rows // batch // GROUP
    sums, _, total = combined(parts)
    total = as_column(total, diagonal(rows))
    result = sums / total
    lines = []
    for b in range(batch):
        at = [b * per * GROUP + i * per + g for g in range(per) for i in range(GROUP)]
        lines.append(jnp.concatenate([result[r : r + 1] for r in at], axis=1))
    out[...] = jnp.concatenate(lines, axis=0).astype(out.dtype)


def on_device(key_cache, value_cache, query, lengths, block_map):
    batch, slots, _, width = key_cache.shape
    row_count, column_count = lax.axis_size("seq_0"), lax.axis_size("seq_1")
    halves = lax.axis_size("head")
    rows = batch * QH // halves + STATS
    anywhere = pl.BlockSpec(memory_space=pl.ANY)
    queries = lax.all_gather(query, "head")
    local = pl.pallas_call(
        attend_kernel,
        out_shape=jax.ShapeDtypeStruct((column_count, halves, rows, HD), jnp.bfloat16),
        in_specs=[pl.BlockSpec(memory_space=pltpu.VMEM), anywhere, anywhere, anywhere, anywhere],
        scratch_shapes=[
            pltpu.VMEM(key_cache.shape, key_cache.dtype),
            pltpu.VMEM(value_cache.shape, value_cache.dtype),
            pltpu.SMEM(block_map.shape, block_map.dtype),
            pltpu.SMEM(lengths.shape, lengths.dtype),
            pltpu.SemaphoreType.DMA((3, 2)),
        ],
        name="attend",
    )(queries, lengths, block_map, key_cache, value_cache)
    parts = local.reshape(column_count * halves, rows, HD)
    parts = lax.all_to_all(parts, ROW, 0, 0, tiled=True)
    parts = pl.pallas_call(
        middle_kernel,
        out_shape=jax.ShapeDtypeStruct((row_count, rows, HD), jnp.bfloat16),
        name="middle",
    )(parts)
    parts = lax.all_to_all(parts, "seq_0", 0, 0, tiled=True)
    return pl.pallas_call(
        last_kernel,
        out_shape=jax.ShapeDtypeStruct(query.shape, query.dtype),
        name="last",
    )(parts)


def solution(mesh):
    torus = Mesh(
        mesh.devices.reshape(mesh.shape["grp"], 16, 8, mesh.shape["head"]),
        ("grp", "seq_0", "seq_1", "head"),
    )
    cache = P("grp", ("seq_0", "seq_1", "head"), None, None)
    placed = (cache, cache, P("grp", "head"), P("grp"), P("grp", None))
    return jax.shard_map(
        on_device, mesh=torus, in_specs=placed, out_specs=P("grp", "head"), check_vma=False
    )
```

```python
import jax
import jax.numpy as jnp
from jax import lax
from jax.experimental import pallas as pl
from jax.experimental.pallas import tpu as pltpu
from jax.sharding import Mesh
from jax.sharding import PartitionSpec as P

QH = 32
KVH = 8
HD = 128
BLK = 128
GROUP = QH // KVH
LOW = -1e30
ROW = ("seq_1", "head")
STATS = 8


def pieces(x):
    first = x.astype(jnp.bfloat16)
    rest = x - first.astype(jnp.float32)
    second = rest.astype(jnp.bfloat16)
    third = (rest - second.astype(jnp.float32)).astype(jnp.bfloat16)
    return first, second, third


def diagonal(rows):
    shape = (rows, HD)
    return lax.broadcasted_iota(jnp.int32, shape, 0) == lax.broadcasted_iota(jnp.int32, shape, 1)


def as_row(column, eye):
    return jnp.sum(jnp.where(eye, column, 0.0), axis=0, keepdims=True)


def as_column(row, eye):
    return jnp.sum(jnp.where(eye, row, 0.0), axis=1, keepdims=True)


def packed(sums, top, total):
    blank = jnp.zeros((STATS - 6, HD), jnp.float32)
    stats = [p.astype(jnp.float32) for p in (*pieces(top), *pieces(total))]
    return jnp.concatenate([sums, *stats, blank], axis=0).astype(jnp.bfloat16)


def attend_kernel(query, lengths, block_map, keys, values, out, key_buf, value_buf, map_buf, len_buf, sems):
    batch, slots = keys.shape[0], keys.shape[1]
    halves = query.shape[0]
    tokens = slots * BLK
    width = keys.shape[3]
    copies = []
    for b in range(batch):
        copies.append(
            (
                pltpu.make_async_copy(keys.at[b], key_buf.at[b], sems.at[0, b]),
                pltpu.make_async_copy(values.at[b], value_buf.at[b], sems.at[1, b]),
            )
        )
    small = (
        pltpu.make_async_copy(block_map, map_buf, sems.at[2, 0]),
        pltpu.make_async_copy(lengths, len_buf, sems.at[2, 1]),
    )
    for copy in small:
        copy.start()
    for pair in copies:
        for copy in pair:
            copy.start()
    for copy in small:
        copy.wait()
    first = lax.axis_index(("seq_0", "seq_1", "head")) * slots
    row_group = lax.broadcasted_iota(jnp.int32, (KVH, width), 0)
    column_group = lax.broadcasted_iota(jnp.int32, (KVH, width), 1) // HD
    own = row_group == column_group
    eye = diagonal(batch * QH // halves)
    sums, tops, totals = [], [], []
    for b in range(batch):
        spread = []
        for i in range(GROUP):
            chunks = []
            for g in range(KVH):
                half, at = divmod(g * GROUP + i, QH // halves)
                chunks.append(query[half, b : b + 1, at * HD : (at + 1) * HD].astype(jnp.float32))
            line = jnp.concatenate(chunks, axis=1)
            spread.append(jnp.where(own, line, 0.0))
        spread = jnp.concatenate(spread, axis=0).astype(jnp.bfloat16)
        limit = len_buf[b] // BLK
        live = jnp.concatenate(
            [
                jnp.full((1, BLK), (map_buf[b, first + j] < limit).astype(jnp.int32))
                for j in range(slots)
            ],
            axis=1,
        )
        live = jnp.broadcast_to(live, (QH, tokens)) > 0
        copies[b][0].wait()
        scores = lax.dot_general(
            spread,
            key_buf[b].reshape(tokens, width),
            (((1,), (1,)), ((), ())),
            preferred_element_type=jnp.float32,
        )
        scores = jnp.where(live, scores * (1.0 / HD**0.5), LOW)
        top = jnp.max(scores, axis=1, keepdims=True)
        expo = jnp.where(live, jnp.exp(scores - top), 0.0)
        total = jnp.sum(expo, axis=1, keepdims=True)
        copies[b][1].wait()
        wide = jnp.dot(
            expo.astype(jnp.bfloat16),
            value_buf[b].reshape(tokens, width),
            preferred_element_type=jnp.float32,
        )
        wide = wide.reshape(GROUP, KVH, width)
        mine = jnp.zeros((GROUP, KVH, HD), jnp.float32)
        for g in range(KVH):
            pick = lax.broadcasted_iota(jnp.int32, mine.shape, 1) == g
            mine = jnp.where(pick, wide[:, :, g * HD : (g + 1) * HD], mine)
        sums.append(mine)
        tops.append(top.reshape(GROUP, KVH, 1))
        totals.append(total.reshape(GROUP, KVH, 1))
    per = KVH // halves
    for half in range(halves):
        part = slice(half * per, (half + 1) * per)

        def gathered(arrays):
            return jnp.concatenate([a[i : i + 1, part].reshape(per, -1) for a in arrays for i in range(GROUP)], axis=0)

        line = packed(
            gathered(sums),
            as_row(gathered(tops), eye),
            as_row(gathered(totals), eye),
        )
        for k in range(out.shape[0]):
            out[k, half] = line


def combined(parts):
    count, rows = parts.shape[0], parts.shape[1] - STATS
    eye = diagonal(rows)
    stats = [parts[:, rows + k, :].astype(jnp.float32) for k in range(6)]
    tops = stats[0] + stats[1] + stats[2]
    totals = stats[3] + stats[4] + stats[5]
    top = jnp.max(tops, axis=0, keepdims=True)
    factors = jnp.exp(tops - top)
    total = jnp.sum(totals * factors, axis=0, keepdims=True)
    sums = jnp.zeros((rows, HD), jnp.float32)
    for n in range(count):
        sums += as_column(factors[n : n + 1], eye) * parts[n, :rows, :].astype(jnp.float32)
    return sums, top, total


def middle_kernel(parts, out):
    line = packed(*combined(parts))
    for k in range(out.shape[0]):
        out[k] = line


def last_kernel(parts, out):
    rows = parts.shape[1] - STATS
    batch = out.shape[0]
    per = rows // batch // GROUP
    sums, _, total = combined(parts)
    total = as_column(total, diagonal(rows))
    result = sums / total
    lines = []
    for b in range(batch):
        at = [b * per * GROUP + i * per + g for g in range(per) for i in range(GROUP)]
        lines.append(jnp.concatenate([result[r : r + 1] for r in at], axis=1))
    out[...] = jnp.concatenate(lines, axis=0).astype(out.dtype)


def near(x):
    return pltpu.with_memory_space_constraint(x, pltpu.VMEM)


def on_device(key_cache, value_cache, query, lengths, block_map):
    batch, slots, _, width = key_cache.shape
    row_count, column_count = lax.axis_size("seq_0"), lax.axis_size("seq_1")
    halves = lax.axis_size("head")
    rows = batch * QH // halves + STATS
    anywhere = pl.BlockSpec(memory_space=pl.ANY)
    queries = lax.all_gather(query, "head")
    local = pl.pallas_call(
        attend_kernel,
        out_shape=pltpu.VMEM((column_count, halves, rows, HD), jnp.bfloat16),
        in_specs=[pl.BlockSpec(memory_space=pltpu.VMEM), anywhere, anywhere, anywhere, anywhere],
        scratch_shapes=[
            pltpu.VMEM(key_cache.shape, key_cache.dtype),
            pltpu.VMEM(value_cache.shape, value_cache.dtype),
            pltpu.SMEM(block_map.shape, block_map.dtype),
            pltpu.SMEM(lengths.shape, lengths.dtype),
            pltpu.SemaphoreType.DMA((3, 2)),
        ],
        name="attend",
    )(near(queries), lengths, block_map, key_cache, value_cache)
    parts = local.reshape(column_count * halves, rows, HD)
    parts = lax.all_to_all(parts, ROW, 0, 0, tiled=True)
    parts = pl.pallas_call(
        middle_kernel,
        out_shape=pltpu.VMEM((row_count, rows, HD), jnp.bfloat16),
        name="middle",
    )(near(parts))
    parts = lax.all_to_all(parts, "seq_0", 0, 0, tiled=True)
    return pl.pallas_call(
        last_kernel,
        out_shape=jax.ShapeDtypeStruct(query.shape, query.dtype),
        name="last",
    )(near(parts))


def solution(mesh):
    torus = Mesh(
        mesh.devices.reshape(mesh.shape["grp"], 16, 8, mesh.shape["head"]),
        ("grp", "seq_0", "seq_1", "head"),
    )
    cache = P("grp", ("seq_0", "seq_1", "head"), None, None)
    placed = (cache, cache, P("grp", "head"), P("grp"), P("grp", None))
    return jax.shard_map(
        on_device, mesh=torus, in_specs=placed, out_specs=P("grp", "head"), check_vma=False
    )
```

```python
import functools

import jax
import jax.numpy as jnp
from jax import lax
from jax.experimental import pallas as pl
from jax.experimental.pallas import tpu as pltpu
from jax.sharding import Mesh
from jax.sharding import PartitionSpec as P

QH = 32
KVH = 8
HD = 128
BLK = 128
GROUP = QH // KVH
LOW = -1e30
ROW = ("seq_1", "head")
STATS = 8


def pieces(x):
    first = x.astype(jnp.bfloat16)
    rest = x - first.astype(jnp.float32)
    second = rest.astype(jnp.bfloat16)
    third = (rest - second.astype(jnp.float32)).astype(jnp.bfloat16)
    return first, second, third


def diagonal(rows):
    shape = (rows, HD)
    return lax.broadcasted_iota(jnp.int32, shape, 0) == lax.broadcasted_iota(jnp.int32, shape, 1)


def as_row(column, eye):
    return jnp.sum(jnp.where(eye, column, 0.0), axis=0, keepdims=True)


def as_column(row, eye):
    return jnp.sum(jnp.where(eye, row, 0.0), axis=1, keepdims=True)


def packed(sums, top, total):
    blank = jnp.zeros((STATS - 6, HD), jnp.float32)
    stats = [p.astype(jnp.float32) for p in (*pieces(top), *pieces(total))]
    return jnp.concatenate([sums, *stats, blank], axis=0).astype(jnp.bfloat16)


def attend_kernel(query, lengths, block_map, keys, values, out, key_buf, value_buf, map_buf, len_buf, sems):
    batch, slots = keys.shape[0], keys.shape[1]
    halves = query.shape[0]
    tokens = slots * BLK
    width = keys.shape[3]
    copies = []
    for b in range(batch):
        copies.append(
            (
                pltpu.make_async_copy(keys.at[b], key_buf.at[b], sems.at[0, b]),
                pltpu.make_async_copy(values.at[b], value_buf.at[b], sems.at[1, b]),
            )
        )
    small = (
        pltpu.make_async_copy(block_map, map_buf, sems.at[2, 0]),
        pltpu.make_async_copy(lengths, len_buf, sems.at[2, 1]),
    )
    for copy in small:
        copy.start()
    for pair in copies:
        for copy in pair:
            copy.start()
    for copy in small:
        copy.wait()
    first = lax.axis_index(("seq_0", "seq_1", "head")) * slots
    row_group = lax.broadcasted_iota(jnp.int32, (KVH, width), 0)
    column_group = lax.broadcasted_iota(jnp.int32, (KVH, width), 1) // HD
    own = row_group == column_group
    eye = diagonal(batch * QH // halves)
    sums, tops, totals = [], [], []
    for b in range(batch):
        spread = []
        for i in range(GROUP):
            chunks = []
            for g in range(KVH):
                half, at = divmod(g * GROUP + i, QH // halves)
                chunks.append(query[half, b : b + 1, at * HD : (at + 1) * HD].astype(jnp.float32))
            line = jnp.concatenate(chunks, axis=1)
            spread.append(jnp.where(own, line, 0.0))
        spread = jnp.concatenate(spread, axis=0).astype(jnp.bfloat16)
        limit = len_buf[b] // BLK
        live = jnp.concatenate(
            [
                jnp.full((1, BLK), (map_buf[b, first + j] < limit).astype(jnp.int32))
                for j in range(slots)
            ],
            axis=1,
        )
        live = jnp.broadcast_to(live, (QH, tokens)) > 0
        copies[b][0].wait()
        scores = lax.dot_general(
            spread,
            key_buf[b].reshape(tokens, width),
            (((1,), (1,)), ((), ())),
            preferred_element_type=jnp.float32,
        )
        scores = jnp.where(live, scores * (1.0 / HD**0.5), LOW)
        top = jnp.max(scores, axis=1, keepdims=True)
        expo = jnp.where(live, jnp.exp(scores - top), 0.0)
        total = jnp.sum(expo, axis=1, keepdims=True)
        copies[b][1].wait()
        wide = jnp.dot(
            expo.astype(jnp.bfloat16),
            value_buf[b].reshape(tokens, width),
            preferred_element_type=jnp.float32,
        )
        wide = wide.reshape(GROUP, KVH, width)
        mine = jnp.zeros((GROUP, KVH, HD), jnp.float32)
        for g in range(KVH):
            pick = lax.broadcasted_iota(jnp.int32, mine.shape, 1) == g
            mine = jnp.where(pick, wide[:, :, g * HD : (g + 1) * HD], mine)
        sums.append(mine)
        tops.append(top.reshape(GROUP, KVH, 1))
        totals.append(total.reshape(GROUP, KVH, 1))
    per = KVH // halves
    for half in range(halves):
        part = slice(half * per, (half + 1) * per)

        def gathered(arrays):
            return jnp.concatenate([a[i : i + 1, part].reshape(per, -1) for a in arrays for i in range(GROUP)], axis=0)

        line = packed(
            gathered(sums),
            as_row(gathered(tops), eye),
            as_row(gathered(totals), eye),
        )
        for k in range(out.shape[0]):
            out[k, half] = line


def combined(parts, held=None):
    count, rows = parts.shape[0], parts.shape[1] - STATS
    eye = diagonal(rows)
    stats = [parts[:, rows + k, :].astype(jnp.float32) for k in range(6)]
    tops = stats[0] + stats[1] + stats[2]
    totals = stats[3] + stats[4] + stats[5]
    if held is not None:
        place = lax.broadcasted_iota(jnp.int32, tops.shape, 0)
        counted = place < 0
        for n in range(count):
            counted |= (place == n) & held[n]
        tops = jnp.where(counted, tops, LOW)
        totals = jnp.where(counted, totals, 0.0)
    top = jnp.max(tops, axis=0, keepdims=True)
    factors = jnp.exp(tops - top)
    if held is not None:
        factors = jnp.where(counted, factors, 0.0)
    total = jnp.sum(totals * factors, axis=0, keepdims=True)
    sums = jnp.zeros((rows, HD), jnp.float32)
    for n in range(count):
        sums += as_column(factors[n : n + 1], eye) * parts[n, :rows, :].astype(jnp.float32)
    return sums, top, total


def middle_kernel(parts, out):
    out[...] = packed(*combined(parts))


def merge_kernel(*refs, receivers):
    *parts, out = refs
    row = lax.axis_index("seq_0")
    held = [row >= 0]
    for rows in receivers:
        got = row < 0
        for r in rows:
            got |= row == r
        held.append(got)
    out[...] = packed(*combined(jnp.stack([p[...] for p in parts]), held))


def last_kernel(parts, out):
    rows = parts.shape[1] - STATS
    batch = out.shape[0]
    per = rows // batch // GROUP
    sums, _, total = combined(parts)
    total = as_column(total, diagonal(rows))
    result = sums / total
    lines = []
    for b in range(batch):
        at = [b * per * GROUP + i * per + g for g in range(per) for i in range(GROUP)]
        lines.append(jnp.concatenate([result[r : r + 1] for r in at], axis=1))
    out[...] = jnp.concatenate(lines, axis=0).astype(out.dtype)


def near(x):
    return pltpu.with_memory_space_constraint(x, pltpu.VMEM)


def on_device(key_cache, value_cache, query, lengths, block_map):
    batch, slots, _, width = key_cache.shape
    row_count, column_count = lax.axis_size("seq_0"), lax.axis_size("seq_1")
    halves = lax.axis_size("head")
    rows = batch * QH // halves + STATS
    anywhere = pl.BlockSpec(memory_space=pl.ANY)
    queries = lax.all_gather(query, "head")
    local = pl.pallas_call(
        attend_kernel,
        out_shape=pltpu.VMEM((column_count, halves, rows, HD), jnp.bfloat16),
        in_specs=[pl.BlockSpec(memory_space=pltpu.VMEM), anywhere, anywhere, anywhere, anywhere],
        scratch_shapes=[
            pltpu.VMEM(key_cache.shape, key_cache.dtype),
            pltpu.VMEM(value_cache.shape, value_cache.dtype),
            pltpu.SMEM(block_map.shape, block_map.dtype),
            pltpu.SMEM(lengths.shape, lengths.dtype),
            pltpu.SemaphoreType.DMA((3, 2)),
        ],
        name="attend",
    )(near(queries), lengths, block_map, key_cache, value_cache)
    row, n = lax.axis_index("seq_0"), row_count
    early, inside, outer = (row >= 1) & (row < n - 4), (row < 4) | (row >= n - 4), row >= 4
    local, row, early, inside, outer = lax.optimization_barrier((local, row, early, inside, outer))
    parts = local.reshape(column_count * halves, rows, HD)
    parts = lax.all_to_all(parts, ROW, 0, 0, tiled=True)
    parts, row, early, inside, outer = lax.optimization_barrier((parts, row, early, inside, outer))
    line = pltpu.VMEM((rows, HD), jnp.bfloat16)
    own = pl.pallas_call(middle_kernel, out_shape=line, name="middle")(near(parts))
    hub = [(n - 4 + k) % n for k in range(8)]
    outside = [r for r in range(n) if r not in hub]

    def merged(receivers, *parts):
        kernel = functools.partial(merge_kernel, receivers=receivers)
        return pl.pallas_call(kernel, out_shape=line, name="merge")(*map(near, parts))

    def moved(x, pairs):
        return lax.ppermute(x, "seq_0", pairs)

    def collected(own):
        pairs = [(8, 7), (6, 5)]
        own = merged([[b for _, b in pairs]], own, moved(own, pairs))
        first, second = [(11, 3), (10, 2), (9, 1)], [(7, 3), (5, 2), (4, 1)]
        to = [b for _, b in first]
        return merged([to, to], own, moved(own, first), moved(own, second))

    own = lax.cond(early, collected, lambda x: x, own)

    def finished(own):
        parts = jnp.broadcast_to(own[None], (len(hub), *own.shape))
        parts = lax.all_to_all(parts, "seq_0", 0, 0, tiled=True, axis_index_groups=[hub, outside])
        return pl.pallas_call(
            last_kernel, out_shape=jax.ShapeDtypeStruct(query.shape, query.dtype), name="last"
        )(near(parts))

    result = lax.cond(inside, finished, lambda x: jnp.zeros(query.shape, query.dtype), own)

    def spread(result):
        near_pairs = [(15, 4), (14, 5), (13, 6), (12, 7)]
        far_pairs = [(15, 8), (14, 9), (13, 10), (12, 11)]
        first, second = moved(result, near_pairs), moved(result, far_pairs)
        return jnp.where(row < 8, first, jnp.where(row < 12, second, result))

    return lax.cond(outer, spread, lambda x: x, result)


def solution(mesh):
    torus = Mesh(
        mesh.devices.reshape(mesh.shape["grp"], 16, 8, mesh.shape["head"]),
        ("grp", "seq_0", "seq_1", "head"),
    )
    cache = P("grp", ("seq_0", "seq_1", "head"), None, None)
    placed = (cache, cache, P("grp", "head"), P("grp"), P("grp", None))
    return jax.shard_map(
        on_device, mesh=torus, in_specs=placed, out_specs=P("grp", "head"), check_vma=False
    )
```

```python
import functools

import jax
import jax.numpy as jnp
from jax import lax
from jax.experimental import pallas as pl
from jax.experimental.pallas import tpu as pltpu
from jax.sharding import Mesh
from jax.sharding import PartitionSpec as P

QH = 32
KVH = 8
HD = 128
BLK = 128
GROUP = QH // KVH
LOW = -1e30
ROW = ("seq_1", "head")
STATS = 8


def pieces(x):
    first = x.astype(jnp.bfloat16)
    rest = x - first.astype(jnp.float32)
    second = rest.astype(jnp.bfloat16)
    third = (rest - second.astype(jnp.float32)).astype(jnp.bfloat16)
    return first, second, third


def diagonal(rows):
    shape = (rows, HD)
    return lax.broadcasted_iota(jnp.int32, shape, 0) == lax.broadcasted_iota(jnp.int32, shape, 1)


def as_row(column, eye):
    return jnp.sum(jnp.where(eye, column, 0.0), axis=0, keepdims=True)


def as_column(row, eye):
    return jnp.sum(jnp.where(eye, row, 0.0), axis=1, keepdims=True)


def packed(sums, top, total):
    blank = jnp.zeros((STATS - 6, HD), jnp.float32)
    stats = [p.astype(jnp.float32) for p in (*pieces(top), *pieces(total))]
    return jnp.concatenate([sums, *stats, blank], axis=0).astype(jnp.bfloat16)


def attend_kernel(query, lengths, block_map, keys, values, out, key_buf, value_buf, map_buf, len_buf, sems):
    batch, slots = keys.shape[0], keys.shape[1]
    halves = query.shape[0]
    tokens = slots * BLK
    width = keys.shape[3]
    copies = []
    for b in range(batch):
        copies.append(
            (
                pltpu.make_async_copy(keys.at[b], key_buf.at[b], sems.at[0, b]),
                pltpu.make_async_copy(values.at[b], value_buf.at[b], sems.at[1, b]),
            )
        )
    small = (
        pltpu.make_async_copy(block_map, map_buf, sems.at[2, 0]),
        pltpu.make_async_copy(lengths, len_buf, sems.at[2, 1]),
    )
    for copy in small:
        copy.start()
    for pair in copies:
        for copy in pair:
            copy.start()
    for copy in small:
        copy.wait()
    first = lax.axis_index(("seq_0", "seq_1", "head")) * slots
    row_group = lax.broadcasted_iota(jnp.int32, (KVH, width), 0)
    column_group = lax.broadcasted_iota(jnp.int32, (KVH, width), 1) // HD
    own = row_group == column_group
    eye = diagonal(batch * QH // halves)
    sums, tops, totals = [], [], []
    for b in range(batch):
        spread = []
        for i in range(GROUP):
            chunks = []
            for g in range(KVH):
                half, at = divmod(g * GROUP + i, QH // halves)
                chunks.append(query[half, b : b + 1, at * HD : (at + 1) * HD].astype(jnp.float32))
            line = jnp.concatenate(chunks, axis=1)
            spread.append(jnp.where(own, line, 0.0))
        spread = jnp.concatenate(spread, axis=0).astype(jnp.bfloat16)
        limit = len_buf[b] // BLK
        live = jnp.concatenate(
            [
                jnp.full((1, BLK), (map_buf[b, first + j] < limit).astype(jnp.int32))
                for j in range(slots)
            ],
            axis=1,
        )
        live = jnp.broadcast_to(live, (QH, tokens)) > 0
        copies[b][0].wait()
        scores = lax.dot_general(
            spread,
            key_buf[b].reshape(tokens, width),
            (((1,), (1,)), ((), ())),
            preferred_element_type=jnp.float32,
        )
        scores = jnp.where(live, scores * (1.0 / HD**0.5), LOW)
        top = jnp.max(scores, axis=1, keepdims=True)
        expo = jnp.where(live, jnp.exp(scores - top), 0.0)
        total = jnp.sum(expo, axis=1, keepdims=True)
        copies[b][1].wait()
        wide = jnp.dot(
            expo.astype(jnp.bfloat16),
            value_buf[b].reshape(tokens, width),
            preferred_element_type=jnp.float32,
        )
        wide = wide.reshape(GROUP, KVH, width)
        mine = jnp.zeros((GROUP, KVH, HD), jnp.float32)
        for g in range(KVH):
            pick = lax.broadcasted_iota(jnp.int32, mine.shape, 1) == g
            mine = jnp.where(pick, wide[:, :, g * HD : (g + 1) * HD], mine)
        sums.append(mine)
        tops.append(top.reshape(GROUP, KVH, 1))
        totals.append(total.reshape(GROUP, KVH, 1))
    per = KVH // halves
    for half in range(halves):
        part = slice(half * per, (half + 1) * per)

        def gathered(arrays):
            return jnp.concatenate([a[i : i + 1, part].reshape(per, -1) for a in arrays for i in range(GROUP)], axis=0)

        line = packed(
            gathered(sums),
            as_row(gathered(tops), eye),
            as_row(gathered(totals), eye),
        )
        for k in range(out.shape[0]):
            out[k, half] = line


def combined(parts, held=None):
    count, rows = parts.shape[0], parts.shape[1] - STATS
    eye = diagonal(rows)
    stats = [parts[:, rows + k, :].astype(jnp.float32) for k in range(6)]
    tops = stats[0] + stats[1] + stats[2]
    totals = stats[3] + stats[4] + stats[5]
    if held is not None:
        place = lax.broadcasted_iota(jnp.int32, tops.shape, 0)
        counted = place < 0
        for n in range(count):
            counted |= (place == n) & held[n]
        tops = jnp.where(counted, tops, LOW)
        totals = jnp.where(counted, totals, 0.0)
    top = jnp.max(tops, axis=0, keepdims=True)
    factors = jnp.exp(tops - top)
    if held is not None:
        factors = jnp.where(counted, factors, 0.0)
    total = jnp.sum(totals * factors, axis=0, keepdims=True)
    sums = jnp.zeros((rows, HD), jnp.float32)
    for n in range(count):
        sums += as_column(factors[n : n + 1], eye) * parts[n, :rows, :].astype(jnp.float32)
    return sums, top, total


def middle_kernel(parts, out):
    out[...] = packed(*combined(parts))


def merge_kernel(*refs, receivers):
    *parts, out = refs
    row = lax.axis_index("seq_0")
    held = [row >= 0]
    for rows in receivers:
        got = row < 0
        for r in rows:
            got |= row == r
        held.append(got)
    out[...] = packed(*combined(jnp.stack([p[...] for p in parts]), held))


def last_kernel(parts, out):
    rows = parts.shape[1] - STATS
    batch = out.shape[0]
    per = rows // batch // GROUP
    sums, _, total = combined(parts)
    total = as_column(total, diagonal(rows))
    result = sums / total
    lines = []
    for b in range(batch):
        at = [b * per * GROUP + i * per + g for g in range(per) for i in range(GROUP)]
        lines.append(jnp.concatenate([result[r : r + 1] for r in at], axis=1))
    out[...] = jnp.concatenate(lines, axis=0).astype(out.dtype)


def near(x):
    return pltpu.with_memory_space_constraint(x, pltpu.VMEM)


def on_device(key_cache, value_cache, query, lengths, block_map):
    batch, slots, _, width = key_cache.shape
    row_count, column_count = lax.axis_size("seq_0"), lax.axis_size("seq_1")
    halves = lax.axis_size("head")
    rows = batch * QH // halves + STATS
    anywhere = pl.BlockSpec(memory_space=pl.ANY)
    queries = lax.all_gather(query, "head")
    local = pl.pallas_call(
        attend_kernel,
        out_shape=pltpu.VMEM((column_count, halves, rows, HD), jnp.bfloat16),
        in_specs=[pl.BlockSpec(memory_space=pltpu.VMEM), anywhere, anywhere, anywhere, anywhere],
        scratch_shapes=[
            pltpu.VMEM(key_cache.shape, key_cache.dtype),
            pltpu.VMEM(value_cache.shape, value_cache.dtype),
            pltpu.SMEM(block_map.shape, block_map.dtype),
            pltpu.SMEM(lengths.shape, lengths.dtype),
            pltpu.SemaphoreType.DMA((3, 2)),
        ],
        name="attend",
    )(near(queries), lengths, block_map, key_cache, value_cache)
    row, n = lax.axis_index("seq_0"), row_count
    line = pltpu.VMEM((rows, HD), jnp.bfloat16)
    out = jax.ShapeDtypeStruct(query.shape, query.dtype)

    def exchanged(local):
        parts = local.reshape(column_count * halves, rows, HD)
        parts = lax.all_to_all(parts, ROW, 0, 0, tiled=True)
        return pl.pallas_call(middle_kernel, out_shape=line, name="middle")(near(parts))

    own = lax.cond(row >= 0, exchanged, lambda x: x[0, 0], local)
    hub = [n - 2, n - 1, 0, 1]
    groups = [hub] + [[r + k for k in range(4)] for r in range(2, n - 2, 4)]
    low, high = n // 4 + 1, n // 2 + 1

    def merged(receivers, *parts):
        kernel = functools.partial(merge_kernel, receivers=receivers)
        return pl.pallas_call(kernel, out_shape=line, name="merge")(*map(near, parts))

    def moved(x, pairs):
        return lax.ppermute(x, "seq_0", pairs)

    def halved(own):
        pairs = [(r + low - 1, r) for r in range(2, low + 1)]
        return merged([[r for _, r in pairs]], own, moved(own, pairs))

    def collected(own):
        senders = [*range(n - 3, high, -1), *range(low, 1, -1)]
        parts = [moved(own, [(r, 1)]) for r in senders]
        return merged([[1]] * len(parts), own, *parts)

    def early(own):
        own = lax.cond((row >= 2) & (row <= high), halved, lambda x: x, own)
        return lax.cond((row <= low) | (row > high), collected, lambda x: x, own)

    own = lax.cond((row >= 1) & (row < n - 2), early, lambda x: x, own)

    def finished(own):
        parts = jnp.broadcast_to(own[None], (len(hub), *own.shape))
        parts = lax.all_to_all(parts, "seq_0", 0, 0, tiled=True, axis_index_groups=groups)
        return pl.pallas_call(last_kernel, out_shape=out, name="last")(near(parts))

    inside = (row < 2) | (row >= n - 2)
    result = lax.cond(inside, finished, lambda x: jnp.zeros(out.shape, out.dtype), own)

    def spread(result):
        for r in range(2, n - 2, 2):

            def passed(x, r=r):
                got = moved(x, [(n - 1, r), (n - 2, r + 1)])
                return jnp.where(row >= n - 2, x, got)

            here = (row >= n - 2) | (row == r) | (row == r + 1)
            result = lax.cond(here, passed, lambda x: x, result)
        return result

    return lax.cond(row >= 2, spread, lambda x: x, result)


def solution(mesh):
    torus = Mesh(
        mesh.devices.reshape(mesh.shape["grp"], 16, 8, mesh.shape["head"]),
        ("grp", "seq_0", "seq_1", "head"),
    )
    cache = P("grp", ("seq_0", "seq_1", "head"), None, None)
    placed = (cache, cache, P("grp", "head"), P("grp"), P("grp", None))
    return jax.shard_map(
        on_device, mesh=torus, in_specs=placed, out_specs=P("grp", "head"), check_vma=False
    )
```
